16 devices in a mesh: replica: 4 (over z, y), pool: 4 (over x, core).
Axes of the slice: x: 2, y: 2, z: 2, core: 2. Of those that a mesh axis runs over, the one named last changes fastest.
Arguments:
- pool: bfloat16 [2, 256, 2, 256, 8, 128], P(None, ('replica', 'pool')), parts along dimension 1
- page_idx: int32 [4, 16, 8], P(None, ('replica', 'pool')), parts along dimension 1
- count: int32 [16, 4], P(('replica', 'pool')), parts along dimension 0
- x: bfloat16 [16, 128, 3072], P(('replica', 'pool')), parts along dimension 0
- norm_attn: bfloat16 [2, 3072], replicated
- wq: bfloat16 [2, 3072, 3072], replicated
- wk: bfloat16 [2, 3072, 1024], replicated
- wv: bfloat16 [2, 3072, 1024], replicated
- wo: bfloat16 [2, 3072, 3072], replicated
- norm_mlp: bfloat16 [2, 3072], replicated
- w_gate: bfloat16 [2, 3072, 8192], replicated
- w_up: bfloat16 [2, 3072, 8192], replicated
- w_down: bfloat16 [2, 8192, 3072], replicated
Outputs:
- output: bfloat16 [16, 128, 3072], P(('replica', 'pool')), parts along dimension 0
There are 4 independent parts. The reference program is written for one: setup_inputs(seed, part) draws one part's arguments, and reference() takes and returns one part's arrays. A program takes and returns all parts, laid end to end along the dimension named above; an argument that names none is the same for every part.
All inputs are finite; a program needn't handle non-finite values.
Results may differ from the reference program's by a relative error of at most 0.0156318.
Values are sent between devices in bfloat16 or wider.
A program may use at most 1.75 GiB of HBM per device.

```python
import jax
import jax.numpy as jnp
from jax import lax

GROUP = 4
LAYERS = 2
TOKENS = 128
SLOTS = 8
PAGES = 16
PAGE = 256
D_MODEL = 3072
HEADS = 24
KV_HEADS = 8
HEAD = 128
FF_WIDTH = 8192
HOT_OWNERS = 1
EPS = 1e-5
ROPE_BASE = 500000.0


def draw_normal(one_key, shape, scale):
    return (jax.random.normal(one_key, shape, jnp.float32) * scale).astype(jnp.bfloat16)


def setup_inputs(seed: int = 0, part: int = 0) -> dict:
    part_key = jax.random.fold_in(jax.random.key(seed), part)
    pool_key, page_key, hot_key, small_key, token_key = jax.random.split(part_key, 5)
    shared = jax.random.split(jax.random.key(seed + 1), 9)
    pool = draw_normal(pool_key, (LAYERS, GROUP * PAGES, 2, PAGE, KV_HEADS, HEAD), 1.0)
    pair_keys = jax.random.split(page_key, GROUP * GROUP)
    picks = jax.vmap(lambda one_key: jax.random.permutation(one_key, PAGES)[:SLOTS])(pair_keys)
    page_idx = picks.reshape(GROUP, GROUP, SLOTS).astype(jnp.int32)
    owner_rank = jax.random.permutation(hot_key, GROUP)
    small_counts = jax.random.randint(small_key, (GROUP, GROUP), 0, SLOTS // 4 + 1)
    count = jnp.where(owner_rank[None, :] < HOT_OWNERS, SLOTS, small_counts).astype(jnp.int32)
    x = draw_normal(token_key, (GROUP, TOKENS, D_MODEL), 1.0)
    attn_width = HEADS * HEAD
    kv_width = KV_HEADS * HEAD
    out_gain = ((GROUP * SLOTS * PAGE // 4 + TOKENS) / 4.0) ** 0.5
    return {
        'pool': pool,
        'page_idx': page_idx,
        'count': count,
        'x': x,
        'norm_attn': (1.0 + 0.2 * jax.random.normal(shared[0], (LAYERS, D_MODEL), jnp.float32)).astype(jnp.bfloat16),
        'wq': draw_normal(shared[1], (LAYERS, D_MODEL, attn_width), D_MODEL ** -0.5),
        'wk': draw_normal(shared[2], (LAYERS, D_MODEL, kv_width), D_MODEL ** -0.5),
        'wv': draw_normal(shared[3], (LAYERS, D_MODEL, kv_width), D_MODEL ** -0.5),
        'wo': draw_normal(shared[4], (LAYERS, attn_width, D_MODEL), out_gain * attn_width ** -0.5),
        'norm_mlp': (1.0 + 0.2 * jax.random.normal(shared[5], (LAYERS, D_MODEL), jnp.float32)).astype(jnp.bfloat16),
        'w_gate': draw_normal(shared[6], (LAYERS, D_MODEL, FF_WIDTH), D_MODEL ** -0.5),
        'w_up': draw_normal(shared[7], (LAYERS, D_MODEL, FF_WIDTH), D_MODEL ** -0.5),
        'w_down': draw_normal(shared[8], (LAYERS, FF_WIDTH, D_MODEL), FF_WIDTH ** -0.5),
    }


def rms_norm(vals, gain):
    vals_f = vals.astype(jnp.float32)
    inv_rms = lax.rsqrt(jnp.mean(vals_f * vals_f, axis=-1, keepdims=True) + EPS)
    return (vals_f * inv_rms * gain.astype(jnp.float32)).astype(jnp.bfloat16)


def rotate(proj, tokens):
    half = proj.shape[-1] // 2
    freqs = ROPE_BASE ** (-jnp.arange(half, dtype=jnp.float32) / half)
    angles = jnp.arange(tokens, dtype=jnp.float32)[:, None] * freqs[None, :]
    cos_t = jnp.cos(angles)[:, None, :]
    sin_t = jnp.sin(angles)[:, None, :]
    first = proj[..., :half]
    second = proj[..., half:]
    return jnp.concatenate([first * cos_t - second * sin_t, second * cos_t + first * sin_t], axis=-1)


def request_layer(x_req, layer_args, count_row, page_rows):
    layer_pool, g_attn, wq_l, wk_l, wv_l, wo_l, g_mlp, wg_l, wu_l, wd_l = layer_args
    tokens = x_req.shape[0]
    q_per_kv = HEADS // KV_HEADS
    prefix_len = GROUP * SLOTS * PAGE
    h_attn = rms_norm(x_req, g_attn)
    q_proj = jnp.dot(h_attn, wq_l, preferred_element_type=jnp.float32).reshape(tokens, HEADS, HEAD)
    k_proj = jnp.dot(h_attn, wk_l, preferred_element_type=jnp.float32).reshape(tokens, KV_HEADS, HEAD)
    q_rot = rotate(q_proj, tokens).astype(jnp.bfloat16)
    k_new = rotate(k_proj, tokens).astype(jnp.bfloat16)
    v_new = jnp.dot(h_attn, wv_l, preferred_element_type=jnp.float32).astype(jnp.bfloat16).reshape(tokens, KV_HEADS, HEAD)
    pages = layer_pool.reshape(GROUP, PAGES, 2, PAGE, KV_HEADS, HEAD)
    fetched = pages[jnp.arange(GROUP)[:, None], page_rows]
    k_all = jnp.concatenate([fetched[:, :, 0].reshape(prefix_len, KV_HEADS, HEAD), k_new], axis=0)
    v_all = jnp.concatenate([fetched[:, :, 1].reshape(prefix_len, KV_HEADS, HEAD), v_new], axis=0)
    slot_ok = jnp.arange(SLOTS)[None, :] < count_row[:, None]
    pre_ok = jnp.broadcast_to(slot_ok[:, :, None], (GROUP, SLOTS, PAGE)).reshape(prefix_len)
    causal = jnp.arange(tokens)[None, :] <= jnp.arange(tokens)[:, None]
    allowed = jnp.concatenate([jnp.broadcast_to(pre_ok[None, :], (tokens, prefix_len)), causal], axis=1)
    q_group = q_rot.reshape(tokens, KV_HEADS, q_per_kv, HEAD)
    scores = jnp.einsum('tgrd,kgd->grtk', q_group.astype(jnp.float32), k_all.astype(jnp.float32)) * (HEAD ** -0.5)
    scores = jnp.where(allowed[None, None], scores, -1e30)
    probs = jax.nn.softmax(scores, axis=-1).astype(jnp.bfloat16)
    attn = jnp.einsum('grtk,kgd->tgrd', probs.astype(jnp.float32), v_all.astype(jnp.float32)).astype(jnp.bfloat16).reshape(tokens, HEADS * HEAD)
    x_mid = (x_req.astype(jnp.float32) + jnp.dot(attn, wo_l, preferred_element_type=jnp.float32)).astype(jnp.bfloat16)
    h_mlp = rms_norm(x_mid, g_mlp)
    gate = jnp.dot(h_mlp, wg_l, preferred_element_type=jnp.float32)
    up_proj = jnp.dot(h_mlp, wu_l, preferred_element_type=jnp.float32)
    gated = (jax.nn.silu(gate) * up_proj).astype(jnp.bfloat16)
    return (x_mid.astype(jnp.float32) + jnp.dot(gated, wd_l, preferred_element_type=jnp.float32)).astype(jnp.bfloat16)


def reference(pool, page_idx, count, x, norm_attn, wq, wk, wv, wo, norm_mlp, w_gate, w_up, w_down):
    layer_stack = (pool, norm_attn, wq, wk, wv, wo, norm_mlp, w_gate, w_up, w_down)

    def one_request(req_args):
        x_req, count_row, page_rows = req_args

        def body(carry, layer_args):
            return request_layer(carry, layer_args, count_row, page_rows), None

        result, unused = lax.scan(body, x_req, layer_stack)
        return result

    return lax.map(one_request, (x, count, page_idx))
```

```python
import functools

import jax
import jax.numpy as jnp
from jax import lax
from jax.experimental import pallas as pl
from jax.experimental.pallas import tpu as pltpu
from jax.sharding import PartitionSpec as P

EPS = 1e-5
ROPE_BASE = 500000.0
NEG = -1e30
LOG2E = 1.4426950408889634

TOKENS = 128
DM = 3072
HEAD = 128
QPK = 3
LANES = QPK * TOKENS
HALF_KV = 4
HALF_Q = HALF_KV * QPK * HEAD
PAGE = 256
PAGES = 16
SLOTS = 8
GROUP = 4
META = GROUP * SLOTS + GROUP
FF = 8192
FF_HALF = FF // 2
SCALE2 = HEAD ** -0.5 * LOG2E

MATE = [(0, 1), (1, 0), (2, 3), (3, 2)]
ACROSS = [(0, 2), (2, 0), (1, 3), (3, 1)]


def params(mb, sem=None):
    return pltpu.CompilerParams(vmem_limit_bytes=mb * 1024 * 1024, dimension_semantics=sem)


def f32dot(lhs, rhs):
    return jnp.dot(lhs, rhs, preferred_element_type=jnp.float32)


def normed(vals, gain):
    vals_f = vals.astype(jnp.float32)
    inv_rms = lax.rsqrt(jnp.mean(vals_f * vals_f, axis=-1, keepdims=True) + EPS)
    return (vals_f * inv_rms * gain.astype(jnp.float32)).astype(jnp.bfloat16)


def prep_body(me, page_ref, mine_ref, mate_ref, scr):
    core = me[0] % 2
    for kv in range(2):
        scr[kv] = page_ref[0, 0, kv].astype(jnp.float32).reshape(PAGE * 8, HEAD)
    for out_ref, half in ((mine_ref, core), (mate_ref, 1 - core)):
        for h in range(HALF_KV):
            rows = pl.ds(half * HALF_KV + h, PAGE, stride=8)
            out_ref[0, 0, h] = scr[0, rows, :].astype(jnp.bfloat16)
            val_t = scr[1, rows, :].T.astype(jnp.bfloat16)
            out_ref[0, 1, h, 0:128, :] = val_t[:, 0:128]
            out_ref[0, 1, h, 128:256, :] = val_t[:, 128:256]


def prep(me, pool, layer):
    shape = jax.ShapeDtypeStruct((PAGES, 2, HALF_KV, PAGE, HEAD), jnp.bfloat16)
    out_spec = pl.BlockSpec((1, 2, HALF_KV, PAGE, HEAD), lambda p, me: (p, 0, 0, 0, 0))
    return pl.pallas_call(
        prep_body,
        name="prep",
        out_shape=(shape, shape),
        grid_spec=pltpu.PrefetchScalarGridSpec(
            num_scalar_prefetch=1,
            grid=(PAGES,),
            in_specs=[pl.BlockSpec((1, 1, 2, PAGE, 8, HEAD), lambda p, me: (layer, p, 0, 0, 0, 0))],
            out_specs=[out_spec, out_spec],
            scratch_shapes=[pltpu.VMEM((2, PAGE * 8, HEAD), jnp.float32)],
        ),
        compiler_params=params(16, ("arbitrary",)),
        cost_estimate=pl.CostEstimate(flops=20_000_000_000, bytes_accessed=33_554_432, transcendentals=0),
    )(me, pool)


def rope_t(proj_t, cos_t, sin_t):
    first = proj_t[0:64]
    second = proj_t[64:128]
    return jnp.concatenate([first * cos_t - second * sin_t, second * cos_t + first * sin_t], axis=0)


def qkv_body(layer, with_kv, me, *refs):
    if with_kv:
        xa, xb, gain, cos_ref, sin_ref, wq, wk, wv, q_out, k_out, v_out, hx = refs
    else:
        xa, xb, gain, cos_ref, sin_ref, wq, q_out, hx = refs

    @pl.when(pl.program_id(0) == 0)
    def _():
        g = gain[layer:layer + 1, :]
        hx[0:TOKENS] = normed(xa[...], g)
        hx[TOKENS:2 * TOKENS] = normed(xb[...], g)

    cos_t = cos_ref[...]
    sin_t = sin_ref[...]
    hv = hx[...]
    q = f32dot(hv, wq[0])
    for r in range(2):
        for j in range(QPK):
            tile = q[r * TOKENS:(r + 1) * TOKENS, j * HEAD:(j + 1) * HEAD]
            q_out[r, 0, :, j * TOKENS:(j + 1) * TOKENS] = rope_t(tile.T, cos_t, sin_t).astype(jnp.bfloat16)
    if with_kv:
        k = f32dot(hv, wk[0])
        v = f32dot(hv, wv[0])
        for r in range(2):
            rows = slice(r * TOKENS, (r + 1) * TOKENS)
            k_out[r, 0] = rope_t(k[rows].T, cos_t, sin_t).T.astype(jnp.bfloat16)
            v_out[r, 0] = v[rows].T.astype(jnp.bfloat16)


def qkv(me, layer, xa, xb, gain, cos_t, sin_t, wq, wk=None, wv=None):
    with_kv = wk is not None
    whole = lambda shape: pl.BlockSpec(shape, lambda h, me: (0,) * len(shape))
    cols = lambda width: pl.BlockSpec((1, DM, width), lambda h, me: (layer, 0, (me[0] % 2) * HALF_KV + h))
    in_specs = [whole((TOKENS, DM)), whole((TOKENS, DM)), whole((2, DM)), whole((64, TOKENS)), whole((64, TOKENS)), cols(QPK * HEAD)]
    out_specs = [pl.BlockSpec((2, 1, HEAD, LANES), lambda h, me: (0, h, 0, 0))]
    out_shape = [jax.ShapeDtypeStruct((2, HALF_KV, HEAD, LANES), jnp.bfloat16)]
    args = [xa, xb, gain, cos_t, sin_t, wq]
    if with_kv:
        in_specs += [cols(HEAD), cols(HEAD)]
        out_specs += [pl.BlockSpec((2, 1, HEAD, HEAD), lambda h, me: (0, h, 0, 0))] * 2
        out_shape += [jax.ShapeDtypeStruct((2, HALF_KV, HEAD, HEAD), jnp.bfloat16)] * 2
        args += [wk, wv]
    flops = 2 * 2 * TOKENS * DM * (HALF_Q + (2 * HALF_KV * HEAD if with_kv else 0))
    return pl.pallas_call(
        functools.partial(qkv_body, layer, with_kv),
        name="qkv",
        out_shape=out_shape,
        grid_spec=pltpu.PrefetchScalarGridSpec(
            num_scalar_prefetch=1,
            grid=(HALF_KV,),
            in_specs=in_specs,
            out_specs=out_specs,
            scratch_shapes=[pltpu.VMEM((2 * TOKENS, DM), jnp.bfloat16)],
        ),
        compiler_params=params(32, ("arbitrary",)),
        cost_estimate=pl.CostEstimate(flops=flops, bytes_accessed=flops // 256, transcendentals=0),
    )(me, *args)


def attn_body(remote, me_ref, meta, *refs):
    if remote:
        q_ref, kv_own, kv_mate, o_ref, ml_ref, buf, acc, ml, sem = refs
    else:
        q_ref, k_new, v_new, kv_own, kv_mate, o_ref, ml_ref, buf, acc, ml, sem = refs
    me = me_ref[0]
    mate = me + 1 - 2 * (me % 2)

    def start(owner_is_me, page, slot):
        @pl.when(owner_is_me)
        def _():
            pltpu.make_async_copy(kv_own.at[page], buf.at[slot], sem.at[slot]).start()

        @pl.when(jnp.logical_not(owner_is_me))
        def _():
            pltpu.make_async_copy(kv_mate.at[page], buf.at[slot], sem.at[slot]).start()

    def request(r, carry):
        base = me if not remote else me + 2 - 4 * (me // 2)
        req = jnp.where(r == 0, base, base + 1 - 2 * (base % 2))
        n_own = meta[req * META + GROUP * SLOTS + me]
        n_all = n_own + meta[req * META + GROUP * SLOTS + mate]

        def fetch(t):
            is_own = t < n_own
            owner = jnp.where(is_own, me, mate)
            j = jnp.where(is_own, t, t - n_own)
            start(is_own, meta[owner * META + req * SLOTS + j], t % 2)

        @pl.when(n_all > 0)
        def _():
            fetch(0)

        for h in range(HALF_KV):
            if remote:
                acc[h] = jnp.zeros((HEAD, LANES), jnp.float32)
                ml[h, 0:1] = jnp.full((1, LANES), NEG, jnp.float32)
                ml[h, 1:2] = jnp.zeros((1, LANES), jnp.float32)
            else:
                s = f32dot(k_new[r, h], q_ref[r, h])
                key = lax.broadcasted_iota(jnp.int32, (TOKENS, LANES), 0)
                tok = lax.broadcasted_iota(jnp.int32, (TOKENS, LANES), 1) % TOKENS
                s = jnp.where(key <= tok, s, NEG)
                m = jnp.max(s, axis=0, keepdims=True)
                p = jnp.exp2((s - m) * SCALE2)
                ml[h, 0:1] = m
                ml[h, 1:2] = jnp.sum(p, axis=0, keepdims=True)
                acc[h] = f32dot(v_new[r, h], p.astype(jnp.bfloat16))

        def unit(t, c):
            slot = t % 2

            @pl.when(t + 1 < n_all)
            def _():
                fetch(t + 1)

            pltpu.make_async_copy(kv_own.at[0], buf.at[slot], sem.at[slot]).wait()
            for h in range(HALF_KV):
                s = f32dot(buf[slot, 0, h], q_ref[r, h])
                m_old = ml[h, 0:1]
                m = jnp.maximum(m_old, jnp.max(s, axis=0, keepdims=True))
                p = jnp.exp2((s - m) * SCALE2)
                keep = jnp.exp2((m_old - m) * SCALE2)
                ml[h, 0:1] = m
                ml[h, 1:2] = ml[h, 1:2] * keep + jnp.sum(p, axis=0, keepdims=True)
                val_t = jnp.concatenate([buf[slot, 1, h, 0:128, :], buf[slot, 1, h, 128:256, :]], axis=1)
                acc[h] = acc[h] * keep + f32dot(val_t, p.astype(jnp.bfloat16))
            return c

        lax.fori_loop(0, n_all, unit, 0)
        for h in range(HALF_KV):
            o_ref[r, h] = acc[h]
            ml_ref[r, h] = ml[h]
        return carry

    lax.fori_loop(0, 2, request, 0)


def attn(me, meta, q, kv_own, kv_mate, k_new=None, v_new=None):
    remote = k_new is None
    vmem = pl.BlockSpec(memory_space=pltpu.VMEM)
    hbm = pl.BlockSpec(memory_space=pltpu.HBM)
    args = [q] if remote else [q, k_new, v_new]
    return pl.pallas_call(
        functools.partial(attn_body, remote),
        name="attn",
        out_shape=(
            jax.ShapeDtypeStruct((2, HALF_KV, HEAD, LANES), jnp.float32),
            jax.ShapeDtypeStruct((2, HALF_KV, 8, LANES), jnp.float32),
        ),
        grid_spec=pltpu.PrefetchScalarGridSpec(
            num_scalar_prefetch=2,
            grid=(),
            in_specs=[vmem] * len(args) + [hbm, hbm],
            out_specs=[vmem, vmem],
            scratch_shapes=[
                pltpu.VMEM((2, 2, HALF_KV, PAGE, HEAD), jnp.bfloat16),
                pltpu.VMEM((HALF_KV, HEAD, LANES), jnp.float32),
                pltpu.VMEM((HALF_KV, 8, LANES), jnp.float32),
                pltpu.SemaphoreType.DMA((2,)),
            ],
        ),
        compiler_params=params(24),
        cost_estimate=pl.CostEstimate(flops=8_000_000_000, bytes_accessed=10_000_000, transcendentals=0),
    )(me, meta, *args, kv_own, kv_mate)


def merge_body(o1, ml1, o2, ml2, a_ref):
    m1, l1 = ml1[0, 0, 0:1], ml1[0, 0, 1:2]
    m2, l2 = ml2[0, 0, 0:1], ml2[0, 0, 1:2]
    m = jnp.maximum(m1, m2)
    w1 = jnp.exp2((m1 - m) * SCALE2)
    w2 = jnp.exp2((m2 - m) * SCALE2)
    inv = 1.0 / (l1 * w1 + l2 * w2)
    out = o1[0, 0] * (w1 * inv) + o2[0, 0] * (w2 * inv)
    for j in range(QPK):
        a_ref[0, :, j * HEAD:(j + 1) * HEAD] = out[:, j * TOKENS:(j + 1) * TOKENS].T.astype(jnp.bfloat16)


def merge(o1, ml1, o2, ml2):
    o_spec = pl.BlockSpec((1, 1, HEAD, LANES), lambda r, h: (r, h, 0, 0))
    ml_spec = pl.BlockSpec((1, 1, 8, LANES), lambda r, h: (r, h, 0, 0))
    return pl.pallas_call(
        merge_body,
        name="merge",
        out_shape=jax.ShapeDtypeStruct((2, TOKENS, HALF_Q), jnp.bfloat16),
        grid=(2, HALF_KV),
        in_specs=[o_spec, ml_spec, o_spec, ml_spec],
        out_specs=pl.BlockSpec((1, TOKENS, LANES), lambda r, h: (r, 0, h)),
        compiler_params=params(8),
    )(o1, ml1, o2, ml2)


WO_BLK = 512


def wo_body(layer, me, a_own, a_mate, xa, xb, gain, wo, x1_ref, h2_ref, scr):
    core = me[0] % 2
    n = pl.program_id(0)

    @pl.when(n == 0)
    def _():
        own = pl.ds(pl.multiple_of(core * HALF_Q, HALF_Q), HALF_Q)
        other = pl.ds(pl.multiple_of((1 - core) * HALF_Q, HALF_Q), HALF_Q)
        scr[0:TOKENS, own] = a_own[0]
        scr[TOKENS:2 * TOKENS, own] = a_own[1]
        scr[0:TOKENS, other] = a_mate[1]
        scr[TOKENS:2 * TOKENS, other] = a_mate[0]

    prod = f32dot(scr[...], wo[0])
    cols = pl.ds(pl.multiple_of(n * WO_BLK, WO_BLK), WO_BLK)
    x1_ref[0:TOKENS, cols] = (xa[...].astype(jnp.float32) + prod[0:TOKENS]).astype(jnp.bfloat16)
    x1_ref[TOKENS:2 * TOKENS, cols] = (xb[...].astype(jnp.float32) + prod[TOKENS:]).astype(jnp.bfloat16)

    @pl.when(n == pl.num_programs(0) - 1)
    def _():
        h2_ref[...] = normed(x1_ref[...], gain[layer:layer + 1, :])


def out_proj(me, layer, a_own, a_mate, xa, xb, gain, wo):
    whole = lambda shape: pl.BlockSpec(shape, lambda n, me: (0,) * len(shape))
    x_spec = pl.BlockSpec((TOKENS, WO_BLK), lambda n, me: (0, n))
    shape = jax.ShapeDtypeStruct((2 * TOKENS, DM), jnp.bfloat16)
    return pl.pallas_call(
        functools.partial(wo_body, layer),
        name="out_proj",
        out_shape=(shape, shape),
        grid_spec=pltpu.PrefetchScalarGridSpec(
            num_scalar_prefetch=1,
            grid=(DM // WO_BLK,),
            in_specs=[
                whole((2, TOKENS, HALF_Q)), whole((2, TOKENS, HALF_Q)), x_spec, x_spec, whole((2, DM)),
                pl.BlockSpec((1, DM, WO_BLK), lambda n, me: (layer, 0, n)),
            ],
            out_specs=[whole((2 * TOKENS, DM)), whole((2 * TOKENS, DM))],
            scratch_shapes=[pltpu.VMEM((2 * TOKENS, DM), jnp.bfloat16)],
        ),
        compiler_params=params(32, ("arbitrary",)),
        cost_estimate=pl.CostEstimate(flops=4_800_000_000, bytes_accessed=20_000_000, transcendentals=0),
    )(me, a_own, a_mate, xa, xb, gain, wo)


FF_BLK = 256


def mlp_body(me, h2, wg, wu, wd, y_own, y_mate):
    hv = h2[...]
    gate = f32dot(hv, wg[0])
    up = f32dot(hv, wu[0])
    gated = (jax.nn.silu(gate) * up).astype(jnp.bfloat16)
    y = f32dot(gated, wd[0])

    @pl.when(pl.program_id(0) == 0)
    def _():
        y_own[...] = y[0:TOKENS]
        y_mate[...] = y[TOKENS:]

    @pl.when(pl.program_id(0) > 0)
    def _():
        y_own[...] += y[0:TOKENS]
        y_mate[...] += y[TOKENS:]


def mlp(me, layer, h2, wg, wu, wd):
    blocks = FF_HALF // FF_BLK
    whole = lambda shape: pl.BlockSpec(shape, lambda n, me: (0,) * len(shape))
    cols = pl.BlockSpec((1, DM, FF_BLK), lambda n, me: (layer, 0, (me[0] % 2) * blocks + n))
    rows = pl.BlockSpec((1, FF_BLK, DM), lambda n, me: (layer, (me[0] % 2) * blocks + n, 0))
    shape = jax.ShapeDtypeStruct((TOKENS, DM), jnp.float32)
    return pl.pallas_call(
        mlp_body,
        name="mlp",
        out_shape=(shape, shape),
        grid_spec=pltpu.PrefetchScalarGridSpec(
            num_scalar_prefetch=1,
            grid=(blocks,),
            in_specs=[whole((2 * TOKENS, DM)), cols, cols, rows],
            out_specs=[whole((TOKENS, DM)), whole((TOKENS, DM))],
        ),
        compiler_params=params(40, ("arbitrary",)),
        cost_estimate=pl.CostEstimate(flops=19_000_000_000, bytes_accessed=76_000_000, transcendentals=0),
    )(me, h2, wg, wu, wd)


def solution(mesh):
    by_request = P(('replica', 'pool'))
    by_owner = P(None, ('replica', 'pool'))
    shared = P()

    def per_device(pool_loc, idx_loc, count_loc, x_loc, norm_attn, wq, wk, wv, wo, norm_mlp, w_gate, w_up, w_down):
        layers = pool_loc.shape[0]
        to_mate = lambda arr: lax.ppermute(arr, 'pool', MATE)
        to_across = lambda arr: lax.ppermute(arr, 'pool', ACROSS)
        me = lax.axis_index('pool').astype(jnp.int32).reshape(1)
        meta = lax.all_gather(jnp.concatenate([idx_loc.reshape(-1), count_loc.reshape(-1)]), 'pool', tiled=True)
        half = HEAD // 2
        freqs = ROPE_BASE ** (-jnp.arange(half, dtype=jnp.float32) / half)
        angles = freqs[:, None] * jnp.arange(TOKENS, dtype=jnp.float32)[None, :]
        cos_t = jnp.cos(angles)
        sin_t = jnp.sin(angles)
        pages = []
        for layer in range(layers):
            mine, theirs = prep(me, pool_loc, layer)
            pages.append((mine, to_mate(theirs)))
        x = x_loc[0]
        for layer in range(layers):
            kv_own, kv_mate = pages[layer]
            x_mate = to_mate(x)
            x_across = to_across(x)
            x_diag = to_mate(x_across)
            q_loc, k_new, v_new = qkv(me, layer, x, x_mate, norm_attn, cos_t, sin_t, wq, wk, wv)
            q_rem, = qkv(me, layer, x_across, x_diag, norm_attn, cos_t, sin_t, wq)
            o_send, ml_send = attn(me, meta, q_rem, kv_own, kv_mate)
            o_rem = to_across(o_send)
            ml_rem = to_across(ml_send)
            o_loc, ml_loc = attn(me, meta, q_loc, kv_own, kv_mate, k_new, v_new)
            a_own = merge(o_loc, ml_loc, o_rem, ml_rem)
            a_mate = to_mate(a_own)
            x1, h2 = out_proj(me, layer, a_own, a_mate, x, x_mate, norm_mlp, wo)
            y_own, y_send = mlp(me, layer, h2, w_gate, w_up, w_down)
            y_got = to_mate(y_send)
            x = (x1[:TOKENS].astype(jnp.float32) + (y_own + y_got)).astype(jnp.bfloat16)
        return x[None]

    return jax.shard_map(per_device, mesh=mesh, in_specs=(by_owner, by_owner, by_request, by_request, shared, shared, shared, shared, shared, shared, shared, shared, shared), out_specs=by_request, check_vma=False)
```

```python
import functools

import jax
import jax.numpy as jnp
from jax import lax
from jax.experimental import pallas as pl
from jax.experimental.pallas import tpu as pltpu
from jax.sharding import PartitionSpec as P


EPS = 1e-5
ROPE_BASE = 500000.0
NEG = -1e30
LOG2E = 1.4426950408889634

TOKENS = 128
DM = 3072
HEAD = 128
QPK = 3
LANES = QPK * TOKENS
HALF_KV = 4
HALF_Q = HALF_KV * QPK * HEAD
PAGE = 256
PAGES = 16
SLOTS = 8
GROUP = 4
META = GROUP * SLOTS + GROUP
FF = 8192
FF_HALF = FF // 2
DEPTH = 4
SCALE2 = HEAD ** -0.5 * LOG2E

MATE = [(0, 1), (1, 0), (2, 3), (3, 2)]
ACROSS = [(0, 2), (2, 0), (1, 3), (3, 1)]


def params(mb, sem=None):
    return pltpu.CompilerParams(vmem_limit_bytes=mb * 1024 * 1024, dimension_semantics=sem)


def f32dot(lhs, rhs):
    return jnp.dot(lhs, rhs, preferred_element_type=jnp.float32)


def normed(vals, gain):
    vals_f = vals.astype(jnp.float32)
    inv_rms = lax.rsqrt(jnp.mean(vals_f * vals_f, axis=-1, keepdims=True) + EPS)
    return (vals_f * inv_rms * gain.astype(jnp.float32)).astype(jnp.bfloat16)


def prep_body(me, page_ref, mine_ref, mate_ref, scr):
    core = me[0] % 2
    for kv in range(2):
        scr[kv] = page_ref[0, 0, kv].astype(jnp.float32).reshape(PAGE * 8, HEAD)
    for out_ref, half in ((mine_ref, core), (mate_ref, 1 - core)):
        for h in range(HALF_KV):
            rows = pl.ds(half * HALF_KV + h, PAGE, stride=8)
            out_ref[0, 0, h] = scr[0, rows, :].astype(jnp.bfloat16)
            val_t = scr[1, rows, :].T.astype(jnp.bfloat16)
            out_ref[0, 1, h, 0:128, :] = val_t[:, 0:128]
            out_ref[0, 1, h, 128:256, :] = val_t[:, 128:256]


def prep(me, pool, layer):
    shape = jax.ShapeDtypeStruct((PAGES, 2, HALF_KV, PAGE, HEAD), jnp.bfloat16)
    out_spec = pl.BlockSpec((1, 2, HALF_KV, PAGE, HEAD), lambda p, me: (p, 0, 0, 0, 0))
    return pl.pallas_call(
        prep_body,
        name="prep",
        out_shape=(shape, shape),
        grid_spec=pltpu.PrefetchScalarGridSpec(
            num_scalar_prefetch=1,
            grid=(PAGES,),
            in_specs=[pl.BlockSpec((1, 1, 2, PAGE, 8, HEAD), lambda p, me: (layer, p, 0, 0, 0, 0))],
            out_specs=[out_spec, out_spec],
            scratch_shapes=[pltpu.VMEM((2, PAGE * 8, HEAD), jnp.float32)],
        ),
        compiler_params=params(60, ("arbitrary",)),
        cost_estimate=pl.CostEstimate(flops=20_000_000_000, bytes_accessed=33_554_432, transcendentals=0),
    )(me, pool)


def rope_t(proj_t, cos_t, sin_t):
    first = proj_t[0:64]
    second = proj_t[64:128]
    return jnp.concatenate([first * cos_t - second * sin_t, second * cos_t + first * sin_t], axis=0)


def qkv_body(layer, with_kv, me, *refs):
    if with_kv:
        xa, xb, gain, cos_ref, sin_ref, wq, wk, wv, q_out, k_out, v_out, hx = refs
    else:
        xa, xb, gain, cos_ref, sin_ref, wq, q_out, hx = refs

    @pl.when(pl.program_id(0) == 0)
    def _():
        g = gain[layer:layer + 1, :]
        hx[0:TOKENS] = normed(xa[...], g)
        hx[TOKENS:2 * TOKENS] = normed(xb[...], g)

    cos_t = cos_ref[...]
    sin_t = sin_ref[...]
    hv = hx[...]
    q = f32dot(hv, wq[0])
    for r in range(2):
        for i in range(PAIR):
            for j in range(QPK):
                col = (i * QPK + j) * HEAD
                tile = q[r * TOKENS:(r + 1) * TOKENS, col:col + HEAD]
                q_out[r, i, :, j * TOKENS:(j + 1) * TOKENS] = rope_t(tile.T, cos_t, sin_t).astype(jnp.bfloat16)
    if with_kv:
        k = f32dot(hv, wk[0])
        v = f32dot(hv, wv[0])
        for r in range(2):
            for i in range(PAIR):
                part = (slice(r * TOKENS, (r + 1) * TOKENS), slice(i * HEAD, (i + 1) * HEAD))
                k_out[r, i] = rope_t(k[part].T, cos_t, sin_t).T.astype(jnp.bfloat16)
                v_out[r, i] = v[part].T.astype(jnp.bfloat16)


PAIR = 2


def qkv(me, layer, xa, xb, gain, cos_t, sin_t, wq, wk=None, wv=None):
    with_kv = wk is not None
    steps = HALF_KV // PAIR
    whole = lambda shape: pl.BlockSpec(shape, lambda h, me: (0,) * len(shape))
    cols = lambda width: pl.BlockSpec((1, DM, width), lambda h, me: (layer, 0, (me[0] % 2) * steps + h))
    in_specs = [whole((TOKENS, DM)), whole((TOKENS, DM)), whole((2, DM)), whole((64, TOKENS)), whole((64, TOKENS)), cols(PAIR * QPK * HEAD)]
    out_specs = [pl.BlockSpec((2, PAIR, HEAD, LANES), lambda h, me: (0, h, 0, 0))]
    out_shape = [jax.ShapeDtypeStruct((2, HALF_KV, HEAD, LANES), jnp.bfloat16)]
    args = [xa, xb, gain, cos_t, sin_t, wq]
    if with_kv:
        in_specs += [cols(PAIR * HEAD), cols(PAIR * HEAD)]
        out_specs += [pl.BlockSpec((2, PAIR, HEAD, HEAD), lambda h, me: (0, h, 0, 0))] * 2
        out_shape += [jax.ShapeDtypeStruct((2, HALF_KV, HEAD, HEAD), jnp.bfloat16)] * 2
        args += [wk, wv]
    flops = 2 * 2 * TOKENS * DM * (HALF_Q + (2 * HALF_KV * HEAD if with_kv else 0))
    return pl.pallas_call(
        functools.partial(qkv_body, layer, with_kv),
        name="qkv",
        out_shape=out_shape,
        grid_spec=pltpu.PrefetchScalarGridSpec(
            num_scalar_prefetch=1,
            grid=(steps,),
            in_specs=in_specs,
            out_specs=out_specs,
            scratch_shapes=[pltpu.VMEM((2 * TOKENS, DM), jnp.bfloat16)],
        ),
        compiler_params=params(40, ("arbitrary",)),
        cost_estimate=pl.CostEstimate(flops=flops, bytes_accessed=flops // 256, transcendentals=0),
    )(me, *args)


def attn_body(places, me_ref, meta, *refs):
    remote = places[0] >= 2
    first = places[0] % 2
    number = len(places)
    if remote:
        q_ref, kv_own, kv_mate, o_ref, buf, acc, ml, s_scr, mx_scr, sem = refs
    else:
        q_ref, k_new, v_new, kv_own, kv_mate, o_ref, buf, acc, ml, s_scr, mx_scr, sem = refs
    me = me_ref[0]
    core = me % 2
    mate = me + 1 - 2 * core
    across = me + 2 - 4 * (me // 2)
    by_place = (me, mate, across, across + 1 - 2 * core)
    reqs = [by_place[place] for place in places]
    n_own = [meta[place * META + GROUP * SLOTS + me] for place in places]
    n_req = [n_own[r] + meta[places[r] * META + GROUP * SLOTS + mate] for r in range(number)]
    total = sum(n_req[1:], n_req[0])

    def fetch(g):
        second = g >= n_req[0]
        t = jnp.where(second, g - n_req[0], g)
        own_count = jnp.where(second, n_own[-1], n_own[0])
        req = jnp.where(second, reqs[-1], reqs[0])
        is_own = t < own_count
        page = meta[jnp.where(is_own, 0, META) + req * SLOTS + jnp.where(is_own, t, t - own_count)]
        slot = g % DEPTH

        @pl.when(jnp.logical_and(g < total, is_own))
        def _():
            pltpu.make_async_copy(kv_own.at[page], buf.at[slot], sem.at[slot]).start()

        @pl.when(jnp.logical_and(g < total, jnp.logical_not(is_own)))
        def _():
            pltpu.make_async_copy(kv_mate.at[page], buf.at[slot], sem.at[slot]).start()

    def arrived(g):
        pltpu.make_async_copy(kv_own.at[0], buf.at[g % DEPTH], sem.at[g % DEPTH]).wait()

    for g in range(DEPTH - 1):
        @pl.when(g < total)
        def _():
            fetch(jnp.int32(g))

    def scores(r, h, slot, to):
        s = f32dot(buf[slot, 0, h], q_ref[first + r, h])
        s_scr[to] = s
        mx_scr[to] = jnp.max(s.reshape(PAGE // 8, 8, LANES), axis=0)

    def request(r, carry):
        count = jnp.where(r == 0, n_req[0], n_req[-1])
        base = jnp.where(r == 0, 0, n_req[0])
        for h in range(HALF_KV):
            if remote:
                acc[h] = jnp.zeros((HEAD, LANES), jnp.float32)
                ml[h, 0:1] = jnp.full((1, LANES), NEG, jnp.float32)
                ml[h, 1:2] = jnp.zeros((1, LANES), jnp.float32)
            else:
                s = f32dot(k_new[r, h], q_ref[r, h])
                key = lax.broadcasted_iota(jnp.int32, (TOKENS, LANES), 0)
                tok = lax.broadcasted_iota(jnp.int32, (TOKENS, LANES), 1) % TOKENS
                s = jnp.where(key <= tok, s, NEG)
                m = jnp.max(s, axis=0, keepdims=True)
                p = jnp.exp2((s - m) * SCALE2)
                ml[h, 0:1] = m
                ml[h, 1:2] = jnp.sum(p, axis=0, keepdims=True)
                acc[h] = f32dot(v_new[r, h], p.astype(jnp.bfloat16))

        @pl.when(count > 0)
        def _():
            arrived(base)
            scores(r, 0, base % DEPTH, 0)

        def unit(t, c):
            g = base + t
            slot = g % DEPTH
            fetch(g + DEPTH - 1)

            @pl.when(t + 1 < count)
            def _():
                arrived(g + 1)

            for h in range(HALF_KV):
                now = h % 2
                scores(r, (h + 1) % HALF_KV, slot if h + 1 < HALF_KV else (g + 1) % DEPTH, 1 - now)
                m_old = ml[h, 0:1]
                m = jnp.maximum(m_old, jnp.max(mx_scr[now], axis=0, keepdims=True))
                p = jnp.exp2((s_scr[now] - m) * SCALE2)
                keep = jnp.exp2((m_old - m) * SCALE2)
                ml[h, 0:1] = m
                ml[h, 1:2] = ml[h, 1:2] * keep + jnp.sum(p, axis=0, keepdims=True)
                val_t = jnp.concatenate([buf[slot, 1, h, 0:128, :], buf[slot, 1, h, 128:256, :]], axis=1)
                acc[h] = acc[h] * keep + f32dot(val_t, p.astype(jnp.bfloat16))
            return c

        lax.fori_loop(0, count, unit, 0)
        for h in range(HALF_KV):
            o_ref[r, h * HEAD:(h + 1) * HEAD] = acc[h]
            o_ref[r, ROWS_O + h:ROWS_O + h + 1] = ml[h, 0:1]
            o_ref[r, ROWS_O + HALF_KV + h:ROWS_O + HALF_KV + h + 1] = ml[h, 1:2]
        return carry

    lax.fori_loop(0, number, request, 0)


ROWS_O = HALF_KV * HEAD
ROWS = ROWS_O + 2 * HALF_KV


def attn(places, me, meta, q, kv_own, kv_mate, k_new=None, v_new=None):
    vmem = pl.BlockSpec(memory_space=pltpu.VMEM)
    hbm = pl.BlockSpec(memory_space=pltpu.HBM)
    args = [q] if k_new is None else [q, k_new, v_new]
    number = len(places)
    return pl.pallas_call(
        functools.partial(attn_body, places),
        name="attn",
        out_shape=jax.ShapeDtypeStruct((number, ROWS, LANES), jnp.float32),
        grid_spec=pltpu.PrefetchScalarGridSpec(
            num_scalar_prefetch=2,
            grid=(),
            in_specs=[vmem] * len(args) + [hbm, hbm],
            out_specs=vmem,
            scratch_shapes=[
                pltpu.VMEM((DEPTH, 2, HALF_KV, PAGE, HEAD), jnp.bfloat16),
                pltpu.VMEM((HALF_KV, HEAD, LANES), jnp.float32),
                pltpu.VMEM((HALF_KV, 8, LANES), jnp.float32),
                pltpu.VMEM((2, PAGE, LANES), jnp.float32),
                pltpu.VMEM((2, 8, LANES), jnp.float32),
                pltpu.SemaphoreType.DMA((DEPTH,)),
            ],
        ),
        compiler_params=params(56),
        cost_estimate=pl.CostEstimate(flops=8_000_000_000 * number, bytes_accessed=5_000_000 * number, transcendentals=0),
    )(me, meta, *args, kv_own, kv_mate)


def merge_body(loc, rem_a, rem_b, a_ref):
    for r, rem in enumerate((rem_a, rem_b)):
        for h in range(HALF_KV):
            top, mid = ROWS_O + h, ROWS_O + HALF_KV + h
            m1, l1 = loc[r, top:top + 1], loc[r, mid:mid + 1]
            m2, l2 = rem[0, top:top + 1], rem[0, mid:mid + 1]
            m = jnp.maximum(m1, m2)
            w1 = jnp.exp2((m1 - m) * SCALE2)
            w2 = jnp.exp2((m2 - m) * SCALE2)
            inv = 1.0 / (l1 * w1 + l2 * w2)
            rows = slice(h * HEAD, (h + 1) * HEAD)
            out = loc[r, rows] * (w1 * inv) + rem[0, rows] * (w2 * inv)
            for j in range(QPK):
                col = (h * QPK + j) * HEAD
                a_ref[r, :, col:col + HEAD] = out[:, j * TOKENS:(j + 1) * TOKENS].T.astype(jnp.bfloat16)


def merge(loc, rem_a, rem_b):
    vmem = pl.BlockSpec(memory_space=pltpu.VMEM)
    return pl.pallas_call(
        merge_body,
        name="merge",
        out_shape=jax.ShapeDtypeStruct((2, TOKENS, HALF_Q), jnp.bfloat16),
        in_specs=[vmem] * 3,
        out_specs=vmem,
        compiler_params=params(16),
        cost_estimate=pl.CostEstimate(flops=1_000_000_000, bytes_accessed=4_000_000, transcendentals=0),
    )(loc, rem_a, rem_b)


WO_BLK = 512
WO_STEPS = DM // WO_BLK
FF_BLK = 256
FF_STEPS = FF_HALF // FF_BLK
DOWN_BLK = 512


def post_body(layer, me, a_own, a_mate, xa, xb, gain, wo, wg, wu, wd, base_ref, send_ref, a_scr, x1, h2):
    core = me[0] % 2
    n = pl.program_id(0)

    @pl.when(n == 0)
    def _():
        own = pl.ds(pl.multiple_of(core * HALF_Q, HALF_Q), HALF_Q)
        other = pl.ds(pl.multiple_of((1 - core) * HALF_Q, HALF_Q), HALF_Q)
        a_scr[0:TOKENS, own] = a_own[0]
        a_scr[TOKENS:2 * TOKENS, own] = a_own[1]
        a_scr[0:TOKENS, other] = a_mate[1]
        a_scr[TOKENS:2 * TOKENS, other] = a_mate[0]

    @pl.when(n < WO_STEPS)
    def _():
        prod = f32dot(a_scr[...], wo[0])
        cols = pl.ds(pl.multiple_of(n * WO_BLK, WO_BLK), WO_BLK)
        x1[0:TOKENS, cols] = (xa[...].astype(jnp.float32) + prod[0:TOKENS]).astype(jnp.bfloat16)
        x1[TOKENS:2 * TOKENS, cols] = (xb[...].astype(jnp.float32) + prod[TOKENS:]).astype(jnp.bfloat16)

    @pl.when(n == WO_STEPS - 1)
    def _():
        h2[...] = normed(x1[...], gain[layer:layer + 1, :])

    @pl.when(n >= WO_STEPS)
    def _():
        first = n == WO_STEPS
        hv = h2[...]
        gate = f32dot(hv, wg[0])
        up = f32dot(hv, wu[0])
        gated = (jax.nn.silu(gate) * up).astype(jnp.bfloat16)
        for d in range(DM // DOWN_BLK):
            cols = slice(d * DOWN_BLK, (d + 1) * DOWN_BLK)
            y = f32dot(gated, wd[0, :, cols])
            base_ref[:, cols] = jnp.where(first, x1[0:TOKENS, cols].astype(jnp.float32), base_ref[:, cols]) + y[0:TOKENS]
            send_ref[:, cols] = jnp.where(first, 0.0, send_ref[:, cols]) + y[TOKENS:]


def post(me, layer, a_own, a_mate, xa, xb, gain, wo, wg, wu, wd):
    whole = lambda shape: pl.BlockSpec(shape, lambda n, me: (0,) * len(shape))
    early = lambda n: jnp.minimum(n, WO_STEPS - 1)
    late = lambda n, me: (me[0] % 2) * FF_STEPS + jnp.maximum(n - WO_STEPS, 0)
    x_spec = pl.BlockSpec((TOKENS, WO_BLK), lambda n, me: (0, early(n)))
    cols = pl.BlockSpec((1, DM, FF_BLK), lambda n, me: (layer, 0, late(n, me)))
    rows = pl.BlockSpec((1, FF_BLK, DM), lambda n, me: (layer, late(n, me), 0))
    shape = jax.ShapeDtypeStruct((TOKENS, DM), jnp.float32)
    act = pltpu.VMEM((2 * TOKENS, DM), jnp.bfloat16)
    return pl.pallas_call(
        functools.partial(post_body, layer),
        name="post",
        out_shape=(shape, shape),
        grid_spec=pltpu.PrefetchScalarGridSpec(
            num_scalar_prefetch=1,
            grid=(WO_STEPS + FF_STEPS,),
            in_specs=[
                whole((2, TOKENS, HALF_Q)), whole((2, TOKENS, HALF_Q)), x_spec, x_spec, whole((2, DM)),
                pl.BlockSpec((1, DM, WO_BLK), lambda n, me: (layer, 0, early(n))), cols, cols, rows,
            ],
            out_specs=[whole((TOKENS, DM)), whole((TOKENS, DM))],
            scratch_shapes=[act, act, act],
        ),
        compiler_params=params(48, ("arbitrary",)),
        cost_estimate=pl.CostEstimate(flops=24_000_000_000, bytes_accessed=95_000_000, transcendentals=0),
    )(me, a_own, a_mate, xa, xb, gain, wo, wg, wu, wd)


def solution(mesh):
    by_request = P(('replica', 'pool'))
    by_owner = P(None, ('replica', 'pool'))
    shared = P()

    def per_device(pool_loc, idx_loc, count_loc, x_loc, norm_attn, wq, wk, wv, wo, norm_mlp, w_gate, w_up, w_down):
        layers = pool_loc.shape[0]
        to_mate = lambda arr: lax.ppermute(arr, 'pool', MATE)
        to_across = lambda arr: lax.ppermute(arr, 'pool', ACROSS)
        me = lax.axis_index('pool').astype(jnp.int32).reshape(1)
        row = jnp.concatenate([idx_loc.reshape(-1), count_loc.reshape(-1)]).reshape(1, META)
        chip = jnp.concatenate([row, to_mate(row)])
        meta = jnp.concatenate([chip, to_across(chip)]).reshape(GROUP * META)
        half = HEAD // 2
        freqs = ROPE_BASE ** (-jnp.arange(half, dtype=jnp.float32) / half)
        angles = freqs[:, None] * jnp.arange(TOKENS, dtype=jnp.float32)[None, :]
        cos_t = jnp.cos(angles)
        sin_t = jnp.sin(angles)
        x = x_loc[0]
        for layer in range(layers):
            x_across = to_across(x)
            x_mate = to_mate(x)
            kv_own, kv_give = prep(me, pool_loc, layer)
            kv_mate = to_mate(kv_give)
            x_diag = to_mate(x_across)
            q_far, = qkv(me, layer, x_across, x_diag, norm_attn, cos_t, sin_t, wq)
            part_a = attn((2,), me, meta, q_far, kv_own, kv_mate)
            got_a = to_across(part_a)
            part_b = attn((3,), me, meta, q_far, kv_own, kv_mate)
            got_b = to_across(part_b)
            q_near, k_new, v_new = qkv(me, layer, x, x_mate, norm_attn, cos_t, sin_t, wq, wk, wv)
            part = attn((0, 1), me, meta, q_near, kv_own, kv_mate, k_new, v_new)
            a_own = merge(part, got_a, got_b)
            a_mate = to_mate(a_own)
            base, y_send = post(me, layer, a_own, a_mate, x, x_mate, norm_mlp, wo, w_gate, w_up, w_down)
            y_got = to_mate(y_send)
            x = (base + y_got).astype(jnp.bfloat16)
        return x[None]

    return jax.shard_map(per_device, mesh=mesh, in_specs=(by_owner, by_owner, by_request, by_request, shared, shared, shared, shared, shared, shared, shared, shared, shared), out_specs=by_request, check_vma=False)
```
